32 devices in a mesh: grp: 2 (over x), tile: 16 (over z, y, core).
Axes of the slice: x: 2, y: 2, z: 4, core: 2. Of those that a mesh axis runs over, the one named last changes fastest.
Arguments:
- visibility: bfloat16 [2, 512, 512, 1024], P(None, 'tile', None, 'grp'), may hold values from -3 to 3, as said below
- dish_pair_okay: int32 [512, 512], P('tile'), may hold values 0 or 1
- triangles: int32 [3, 32768], P(None, 'tile'), may hold values from 0 to 511, as said below
Outputs:
- triangle_means: float32 [2, 32768], P(None, 'tile')
- closure_spectrum: float32 [2, 1024], P(None, ('grp', 'tile'))
The draws below stay inside these ranges and needn't reach their ends.
Inputs may be any that keep to these rules, and one draw needn't show every extreme that they name: Both parts of every visibility lie in -3 to 3. `triangles`: column j belongs to block d = j // 2048 and level k = (j % 2048) // 1024; its first antenna lies in block d (antennas d * 32 to d * 32 + 31), its second in block d XOR 2**k, and its third is any antenna other than the first two.
All inputs are finite; a program needn't handle non-finite values. No bound on the sum of `dish_pair_okay` on one device may be relied on, other than what follows from the above.
Results may differ from the reference program's by a relative error of at most 0.0003.
Values may be sent and summed in bfloat16 or wider, within the bound.
A program may use at most 128 MiB of HBM per device.

```python
import math
import jax
import jax.numpy as jnp
from jax import lax

RECEIVER_DISHES = 512
RADIO_BANDS = 1024
TRI_LVL = 1024
TA = 32
TRI_DEV = 2048
THREE_DISH_SETS = 32768


def draw_visibility(key, part):
    seed_sequence = jax.random.split(key, 3)
    rotation_angles = jax.random.uniform(seed_sequence[0], (RECEIVER_DISHES, RADIO_BANDS), jnp.float32, -math.pi, math.pi)
    loudness_scale = 0.8 + 0.4 * jax.random.uniform(seed_sequence[1], (RECEIVER_DISHES, RADIO_BANDS), jnp.float32)
    hiss_component = 0.3 * jnp.clip(jax.random.normal(seed_sequence[2], (2, RECEIVER_DISHES, RECEIVER_DISHES, RADIO_BANDS), jnp.float32), -4.0, 4.0)
    gain_real = loudness_scale * jnp.cos(rotation_angles)
    gain_imag = loudness_scale * jnp.sin(rotation_angles)
    signal_real = gain_real[:, None, :] * gain_real[None, :, :] + gain_imag[:, None, :] * gain_imag[None, :, :]
    signal_imag = gain_imag[:, None, :] * gain_real[None, :, :] - gain_real[:, None, :] * gain_imag[None, :, :]
    return (jnp.stack([signal_real, signal_imag]) + hiss_component).astype(jnp.bfloat16)


def draw_triangles(key, part):
    seed_sequence = jax.random.split(key, 3)
    column = jnp.arange(THREE_DISH_SETS, dtype=jnp.int32)
    block_index = column // TRI_DEV
    level_index = column % TRI_DEV // TRI_LVL
    partner = jnp.bitwise_xor(block_index, jnp.left_shift(jnp.ones_like(level_index), level_index))
    first = block_index * TA + jax.random.randint(seed_sequence[0], (THREE_DISH_SETS,), 0, TA, jnp.int32)
    second = partner * TA + jax.random.randint(seed_sequence[1], (THREE_DISH_SETS,), 0, TA, jnp.int32)
    lower = jnp.minimum(first, second)
    upper = jnp.maximum(first, second)
    vertex_point = jax.random.randint(seed_sequence[2], (THREE_DISH_SETS,), 0, RECEIVER_DISHES - 2, jnp.int32)
    vertex_point = vertex_point + (vertex_point >= lower).astype(jnp.int32)
    vertex_point = vertex_point + (vertex_point >= upper).astype(jnp.int32)
    return jnp.stack([first, second, vertex_point]).astype(jnp.int32)


def place_ends(result, own_key, low, largest):
    spot = [jax.random.randint(jax.random.fold_in(own_key, axis), (), 0, length) for axis, length in enumerate(result.shape)]
    widest = result.shape.index(max(result.shape))
    beside = spot[:widest] + [(spot[widest] + 1) % result.shape[widest]] + spot[widest + 1:]
    return result.at[tuple(spot)].set(low).at[tuple(beside)].set(largest)


def setup_inputs(seed: int = 0) -> dict:
    seeds = jax.random.split(jax.random.key(seed), 4)
    return {
        "visibility": draw_visibility(jax.random.fold_in(seeds[3], 71), 0),
        "dish_pair_okay": place_ends((jax.random.randint(seeds[1], (RECEIVER_DISHES, RECEIVER_DISHES), 0, 8) < 7).astype(jnp.int32), jax.random.fold_in(seeds[1], 1), 0, 1),
        "triangles": draw_triangles(jax.random.fold_in(seeds[3], 71), 0),
    }


def bispectrum(edge_ab, edge_bc, edge_ac):
    edge_ab = edge_ab.astype(jnp.float32)
    edge_bc = edge_bc.astype(jnp.float32)
    edge_ac = edge_ac.astype(jnp.float32)
    prod_real = edge_ab[0] * edge_bc[0] - edge_ab[1] * edge_bc[1]
    prod_imag = edge_ab[0] * edge_bc[1] + edge_ab[1] * edge_bc[0]
    real_part = prod_real * edge_ac[0] + prod_imag * edge_ac[1]
    imag_part = prod_imag * edge_ac[0] - prod_real * edge_ac[1]
    return (real_part, imag_part)

def reference(visibility, dish_pair_okay, triangles):
    flag_table = dish_pair_okay.astype(jnp.float32)
    count = triangles.shape[1] // TRI_LVL
    blocks = jnp.transpose(triangles.reshape(3, count, TRI_LVL), (1, 0, 2))

    def step(carry, block):
        first, second, vertex_point = (block[0], block[1], block[2])
        edge_ab = visibility[:, first, second, :]
        edge_bc = visibility[:, second, vertex_point, :]
        edge_ac = visibility[:, first, vertex_point, :]
        weight = flag_table[first, second] * flag_table[second, vertex_point] * flag_table[first, vertex_point]
        real_part, imag_part = bispectrum(edge_ab, edge_bc, edge_ac)
        weighted_real = weight[:, None] * real_part
        weighted_imag = weight[:, None] * imag_part
        magnitude = weight[:, None] * jnp.sqrt(real_part * real_part + imag_part * imag_part)
        new_carry = (carry[0] + lax.optimization_barrier(jnp.sum(weighted_real, 0)), carry[1] + lax.optimization_barrier(jnp.sum(weighted_imag, 0)), carry[2] + lax.optimization_barrier(jnp.sum(magnitude, 0)))
        means = jnp.stack([lax.optimization_barrier(jnp.sum(weighted_real, 1)), lax.optimization_barrier(jnp.sum(weighted_imag, 1))]) / RADIO_BANDS
        return (new_carry, means)
    start = (jnp.zeros((RADIO_BANDS,), jnp.float32), jnp.zeros((RADIO_BANDS,), jnp.float32), jnp.zeros((RADIO_BANDS,), jnp.float32))
    totals, means = lax.scan(step, start, blocks)
    triangle_means = jnp.transpose(means, (1, 0, 2)).reshape(2, count * TRI_LVL)
    closure_spectrum = jnp.stack([totals[0], totals[1]]) / (1.0 + totals[2])
    return (triangle_means, closure_spectrum)
```

```python
import functools

import jax
import jax.numpy as jnp
from jax import lax
from jax.experimental import pallas as pl
from jax.experimental.pallas import tpu as pltpu
from jax.sharding import PartitionSpec as P

TRI_LVL = 1024
LANES = 128
SIDE = 256
FAR = 128
MESH = pl.DeviceIdType.MESH


def dot(a, b):
    return lax.dot_general(a, b, (((1,), (0,)), ((), ())), preferred_element_type=jnp.float32)


def fold(x):
    total = x[:8]
    for i in range(1, x.shape[0] // 8):
        total = total + x[i * 8 : i * 8 + 8]
    return total


def mega_kernel(
    vis,
    okay,
    tri,
    means,
    closure,
    table,
    ring,
    spread,
    gather,
    asked,
    got,
    ask_rows,
    own_rows,
    ask_smem,
    own_smem,
    bc_send,
    bc_recv,
    pair,
    prod,
    line,
    sums,
    spec_acc,
    spec_out,
    spec_recv,
    ring_sem,
    move_sem,
    idx_send,
    idx_recv,
    near_send,
    near_recv,
    far_send,
    far_recv,
    sum_send,
    sum_recv,
    spec_send_sem,
    spec_recv_sem,
    *,
    groups,
    tiles,
    levels,
    step_rows,
):
    _, dishes, cols, channels = vis.shape
    chunks = channels // LANES
    kinds = 2 * chunks
    block = SIDE // kinds
    blank = dishes * cols
    count = tri.shape[1] // levels
    packs = count // LANES
    last = levels - 1
    slots = ring.shape[0]
    steps = dishes // step_rows
    pieces = count // FAR
    width = channels // tiles
    me_g, me = lax.axis_index("grp"), lax.axis_index("tile")
    peers = [(lax.rem(me_g + k, groups), me) for k in range(1, groups)]
    others = [(me_g, lax.rem(me + k, tiles)) for k in range(1, tiles)]
    partner = [(me_g, jnp.bitwise_xor(me, 1 << level)) for level in range(levels)]

    barrier = pltpu.get_barrier_semaphore()
    for device in peers + others:
        pl.semaphore_signal(barrier, inc=1, device_id=device, device_id_type=MESH)

    def fetch(s, slot):
        return pltpu.make_async_copy(vis.at[:, pl.ds(s * step_rows, step_rows)], ring.at[slot], ring_sem.at[slot])

    for s in range(slots - 1):
        fetch(s, s).start()

    def remote(src, dst, send, recv, device):
        return pltpu.make_async_remote_copy(
            src_ref=src, dst_ref=dst, send_sem=send, recv_sem=recv, device_id=device, device_id_type=MESH
        )

    out_at = lax.broadcasted_iota(jnp.int32, (SIDE, SIDE), 0)
    in_at = lax.broadcasted_iota(jnp.int32, (SIDE, SIDE), 1)
    one, nil = jnp.ones((), jnp.float32), jnp.zeros((), jnp.float32)
    spread[...] = jnp.where(in_at == lax.rem(out_at, kinds) * block + out_at // kinds, one, nil).astype(spread.dtype)
    gather[...] = jnp.where(in_at == lax.rem(out_at, block) * kinds + out_at // block, one, nil).astype(gather.dtype)
    table[blank] = jnp.zeros((kinds, LANES), table.dtype)
    spec_acc[...] = jnp.zeros(spec_acc.shape, spec_acc.dtype)

    flags = okay[...].astype(jnp.float32).astype(jnp.bfloat16)

    def look_up(first, seconds):
        n = first.shape[1]
        hot = jnp.where(lax.broadcasted_iota(jnp.int32, (dishes, n), 0) == first, one, nil).astype(jnp.bfloat16)
        rows = lax.dot_general(flags, hot, (((0,), (0,)), ((), ())), preferred_element_type=jnp.float32)
        at = lax.broadcasted_iota(jnp.int32, (cols, n), 0)
        good = None
        for second in seconds:
            hit = jnp.sum(jnp.where(at == second, rows, 0.0), 0, keepdims=True)
            good = hit if good is None else good * hit
        return good

    for level in range(levels):
        for i in range(packs):
            at = level * count + i * LANES
            a, b, c = [tri[pl.ds(e, 1), pl.ds(at, LANES)] for e in range(3)]
            first = a - me * dishes
            second = b - jnp.bitwise_xor(me, 1 << level) * dishes
            good = look_up(first, (b, c)) > 0.5
            asked[level, pl.ds(i, 1), :] = jnp.clip(jnp.where(good, second * cols + c, blank), 0, blank)
            own_rows[level, 0, pl.ds(i, 1), :] = jnp.clip(first * cols + b, 0, blank)
            own_rows[level, 1, pl.ds(i, 1), :] = jnp.clip(first * cols + c, 0, blank)

    def turn(s):
        slot = lax.rem(s, slots)
        fetch(s, slot).wait()
        for a in range(step_rows):
            for u in range(cols // (2 * block)):
                base = u * 2 * block
                x = jnp.concatenate(
                    [
                        jnp.concatenate(
                            [
                                ring[slot, plane, a, pl.ds(base + g * block, block), pl.ds(c * LANES, LANES)]
                                for c in range(chunks)
                                for plane in range(2)
                            ],
                            0,
                        )
                        for g in range(2)
                    ],
                    1,
                )
                y = dot(spread[...], x)
                for g in range(2):
                    rows = y[:, g * LANES : (g + 1) * LANES].reshape(block, kinds, LANES)
                    table[pl.ds((s * step_rows + a) * cols + base + g * block, block)] = rows.astype(table.dtype)

    def turn_step(s, _):
        @pl.when(s + slots - 1 < steps)
        def _():
            fetch(s + slots - 1, lax.rem(s + slots - 1, slots)).start()

        turn(s)
        return 0

    lax.fori_loop(0, 1, turn_step, 0)
    pl.semaphore_wait(barrier, len(peers) + len(others))
    ask = [
        remote(asked.at[level], got.at[level], idx_send.at[level], idx_recv.at[level], partner[level])
        for level in range(levels)
    ]
    for copy in ask:
        copy.start()
    lax.fori_loop(1, steps, turn_step, 0)

    move_own = pltpu.make_async_copy(own_rows, own_smem, move_sem.at[levels])
    move_own.start()
    moves = []
    for level in reversed(range(levels)):
        ask[level].wait()
        for i in range(packs):
            row = got[level, pl.ds(i, 1), :]
            first, second = row // cols, lax.rem(row, cols)
            good = look_up(first, (second,)) > 0.5
            ask_rows[level, pl.ds(i, 1), :] = jnp.clip(jnp.where(good, row, blank), 0, blank)
        move = pltpu.make_async_copy(ask_rows.at[level], ask_smem.at[level], move_sem.at[level])
        move.start()
        moves.append(move)

    def take(level, start, n):
        unroll = 32

        def some(it, _):
            for u in range(unroll):
                j = start + it * unroll + u
                bc_send[level, j] = table[ask_smem[level, j // LANES, lax.rem(j, LANES)]]
            return 0

        lax.fori_loop(0, n // unroll, some, 0)

    far = [
        remote(
            bc_send.at[last, pl.ds(k * FAR, FAR)],
            bc_recv.at[last, pl.ds(k * FAR, FAR)],
            far_send.at[k],
            far_recv.at[k],
            partner[last],
        )
        for k in range(pieces)
    ]
    moves[0].wait()
    for k in range(pieces):
        take(last, k * FAR, FAR)
        if k > 0:
            far[k - 1].start()
    near = [
        remote(bc_send.at[level], bc_recv.at[level], near_send.at[level], near_recv.at[level], partner[level])
        for level in range(last)
    ]
    for move in moves[1:]:
        move.wait()
    for level in range(last):
        take(level, 0, count)
        if level == 0:
            far[pieces - 1].start()
    move_own.wait()
    for copy in near:
        copy.start()

    def products(level, n_blocks):
        def some(it, _):
            for s in range(n_blocks):
                start = (it * n_blocks + s) * block
                for u in range(block):
                    j = start + u
                    for e in range(2):
                        row = table[own_smem[level, e, j // LANES, lax.rem(j, LANES)]]
                        pair[s, e, pl.ds(u * kinds, kinds), :] = row
            for s in range(n_blocks):
                start = pl.multiple_of((it * n_blocks + s) * block, block)
                y = dot(gather[...], jnp.concatenate([pair[s, 0], pair[s, 1]], 1))
                for c in range(chunks):
                    at = 2 * c * block
                    a_r, a_i = y[at : at + block, :LANES], y[at + block : at + 2 * block, :LANES]
                    c_r, c_i = y[at : at + block, LANES:], y[at + block : at + 2 * block, LANES:]
                    prod[level, 0, c, pl.ds(start, block), :] = a_r * c_r + a_i * c_i
                    prod[level, 1, c, pl.ds(start, block), :] = a_i * c_r - a_r * c_i
            return 0

        lax.fori_loop(0, count // (n_blocks * block), some, 0)

    def bispectra(level, start, n):
        wide = min(2, n // block)
        acc = [None] * (3 * chunks)
        for s in range(n // (wide * block)):
            begin = pl.multiple_of(start + s * wide * block, wide * block)
            x = [bc_recv[level, pl.ds(begin + g * block, block)].reshape(SIDE, LANES) for g in range(wide)]
            y = dot(gather[...], jnp.concatenate(x, 1) if wide > 1 else x[0])
            for g in range(wide):
                lanes = slice(g * LANES, (g + 1) * LANES)
                rows = pl.ds(begin + g * block, block)
                total_r = total_i = None
                for c in range(chunks):
                    at = 2 * c * block
                    b_r, b_i = y[at : at + block, lanes], y[at + block : at + 2 * block, lanes]
                    w_r, w_i = prod[level, 0, c, rows, :], prod[level, 1, c, rows, :]
                    real = w_r * b_r - w_i * b_i
                    imag = w_r * b_i + w_i * b_r
                    norm = jnp.sqrt(real * real + imag * imag)
                    for part, value in enumerate((real, imag, norm)):
                        value = fold(value)
                        old = acc[3 * c + part]
                        acc[3 * c + part] = value if old is None else old + value
                    total_r = real if c == 0 else total_r + real
                    total_i = imag if c == 0 else total_i + imag
                line[0, pl.ds(s * wide * block + g * block, block), :] = total_r
                line[1, pl.ds(s * wide * block + g * block, block), :] = total_i
        for c in range(chunks):
            for part in range(3):
                spec_acc[c, part] = spec_acc[c, part] + acc[3 * c + part]
        ones = jnp.ones((8, LANES), jnp.float32)
        for part in range(2):
            lane_sum = lax.dot_general(
                ones,
                line[part, pl.ds(0, n), :],
                (((1,), (1,)), ((), ())),
                precision=lax.Precision.HIGHEST,
                preferred_element_type=jnp.float32,
            )
            sums[0, level, pl.ds(part, 1), pl.ds(pl.multiple_of(start, LANES), n)] = lane_sum[:1]

    products(0, 4 * 32 // block)
    for level in range(1, levels):
        products(level, 4 * 32 // block)
    for level in range(last):
        near[level].wait()
        lax.fori_loop(0, count // 256, lambda it, _, level=level: (bispectra(level, it * 256, 256), 0)[1], 0)
    early = [
        remote(sums.at[0, level], sums.at[k, level], sum_send.at[k, level], sum_recv.at[k, level], device)
        for k, device in enumerate(peers, 1)
        for level in range(last)
    ]
    for k in range(pieces):
        far[k].wait()
        bispectra(last, k * FAR, FAR)
        if k == 0:
            for copy in early:
                copy.start()
    copies = list(early)
    for k, device in enumerate(peers, 1):
        copies.append(remote(sums.at[0, last], sums.at[k, last], sum_send.at[k, last], sum_recv.at[k, last], device))
        copies[-1].start()
    for c in range(chunks):
        for part in range(3):
            spec_out[c, pl.ds(part, 1), :] = jnp.sum(spec_acc[c, part], 0, keepdims=True)
    spread_out = []
    for k, device in enumerate(others, 1):
        spread_out.append(
            remote(
                spec_out.at[device[1] * width // LANES],
                spec_recv.at[k],
                spec_send_sem.at[k],
                spec_recv_sem.at[k],
                device,
            )
        )
        spread_out[-1].start()
    for copy in copies:
        copy.wait()
    bands = channels * groups
    for level in range(levels):
        total = sums[0, level]
        for k in range(1, groups):
            total = total + sums[k, level]
        means[:, pl.ds(level * count, count)] = total / bands
    for copy in spread_out:
        copy.wait()
    total = spec_out[me * width // LANES]
    for k in range(1, tiles):
        total = total + spec_recv[k]
    closure[...] = total[:2] / (1.0 + total[2:3])


def body(visibility, dish_pair_okay, triangles):
    _, dishes, cols, channels = visibility.shape
    levels = triangles.shape[1] // TRI_LVL
    tiles, groups = lax.axis_size("tile"), lax.axis_size("grp")
    chunks = channels // LANES
    kinds = 2 * chunks
    packs = TRI_LVL // LANES
    step_rows, slots = 4, 3
    pieces = TRI_LVL // FAR
    width = channels // tiles
    vmem = pl.BlockSpec(memory_space=pltpu.VMEM)
    f32, bf16, i32 = jnp.float32, jnp.bfloat16, jnp.int32
    dma = pltpu.SemaphoreType.DMA
    triangle_means, closure = pl.pallas_call(
        functools.partial(mega_kernel, groups=groups, tiles=tiles, levels=levels, step_rows=step_rows),
        in_specs=[pl.BlockSpec(memory_space=pl.ANY), vmem, vmem],
        out_specs=[vmem, vmem],
        out_shape=[
            jax.ShapeDtypeStruct((2, triangles.shape[1]), f32),
            jax.ShapeDtypeStruct((2, LANES), f32),
        ],
        scratch_shapes=[
            pltpu.VMEM((dishes * cols + 1, kinds, LANES), bf16),
            pltpu.VMEM((slots, 2, step_rows, cols, channels), bf16),
            pltpu.VMEM((SIDE, SIDE), bf16),
            pltpu.VMEM((SIDE, SIDE), bf16),
            pltpu.VMEM((levels, packs, LANES), i32),
            pltpu.VMEM((levels, packs, LANES), i32),
            pltpu.VMEM((levels, packs, LANES), i32),
            pltpu.VMEM((levels, 2, packs, LANES), i32),
            pltpu.SMEM((levels, packs, LANES), i32),
            pltpu.SMEM((levels, 2, packs, LANES), i32),
            pltpu.VMEM((levels, TRI_LVL, kinds, LANES), bf16),
            pltpu.VMEM((levels, TRI_LVL, kinds, LANES), bf16),
            pltpu.VMEM((4, 2, SIDE, LANES), bf16),
            pltpu.VMEM((levels, 2, chunks, TRI_LVL, LANES), f32),
            pltpu.VMEM((2, 256, LANES), f32),
            pltpu.VMEM((groups, levels, 2, TRI_LVL), f32),
            pltpu.VMEM((chunks, 3, 8, LANES), f32),
            pltpu.VMEM((chunks, 8, LANES), f32),
            pltpu.VMEM((tiles, 8, LANES), f32),
            dma((slots,)),
            dma((levels + 1,)),
            dma((levels,)),
            dma((levels,)),
            dma((levels,)),
            dma((levels,)),
            dma((pieces,)),
            dma((pieces,)),
            dma((groups, levels)),
            dma((groups, levels)),
            dma((tiles,)),
            dma((tiles,)),
        ],
        compiler_params=pltpu.CompilerParams(
            collective_id=0, has_side_effects=True, vmem_limit_bytes=67043328
        ),
        name="bispectra",
    )(visibility, dish_pair_okay, triangles)
    at = lax.rem(lax.axis_index("tile") * width, LANES)
    return (triangle_means, lax.dynamic_slice_in_dim(closure, at, width, 1))


def solution(mesh):
    return jax.shard_map(
        body,
        mesh=mesh,
        in_specs=(P(None, "tile", None, "grp"), P("tile", None), P(None, "tile")),
        out_specs=(P(None, "tile"), P(None, ("grp", "tile"))),
        check_vma=False,
    )
```

```python
import functools

import jax
import jax.numpy as jnp
from jax import lax
from jax.experimental import pallas as pl
from jax.experimental.pallas import tpu as pltpu
from jax.sharding import PartitionSpec as P

TRI_LVL = 1024
LANES = 128
SIDE = 256
FAR = 128
MESH = pl.DeviceIdType.MESH


def dot(a, b):
    return lax.dot_general(a, b, (((1,), (0,)), ((), ())), preferred_element_type=jnp.float32)


def fold(x):
    total = x[:8]
    for i in range(1, x.shape[0] // 8):
        total = total + x[i * 8 : i * 8 + 8]
    return total


def far_room(count):
    return count * 3 // 4 // FAR * FAR


def mega_kernel(
    vis,
    okay,
    tri,
    means,
    closure,
    table,
    ring,
    spread,
    gather,
    asked,
    got,
    good_out,
    good_in,
    far_rows,
    hot,
    excess,
    own_rows,
    ask_smem,
    own_smem,
    bc_send,
    bc_recv,
    pair,
    prod,
    line,
    sums,
    spec_acc,
    spec_out,
    spec_recv,
    ring_sem,
    move_sem,
    idx_send,
    idx_recv,
    good_send,
    good_recv,
    near_send,
    near_recv,
    far_send,
    far_recv,
    sum_send,
    sum_recv,
    spec_send_sem,
    spec_recv_sem,
    *,
    groups,
    tiles,
    levels,
    step_rows,
):
    _, dishes, cols, channels = vis.shape
    chunks = channels // LANES
    kinds = 2 * chunks
    block = SIDE // kinds
    blank = dishes * cols
    count = tri.shape[1] // levels
    packs = count // LANES
    last = levels - 1
    slots = ring.shape[0]
    steps = dishes // step_rows
    room = far_room(count)
    pieces = room // FAR
    width = channels // tiles
    me_g, me = lax.axis_index("grp"), lax.axis_index("tile")
    peers = [(lax.rem(me_g + k, groups), me) for k in range(1, groups)]
    others = [(me_g, lax.rem(me + k, tiles)) for k in range(1, tiles)]
    partner = [(me_g, jnp.bitwise_xor(me, 1 << level)) for level in range(levels)]

    barrier = pltpu.get_barrier_semaphore()
    for device in peers + others:
        pl.semaphore_signal(barrier, inc=1, device_id=device, device_id_type=MESH)

    def fetch(s, slot):
        return pltpu.make_async_copy(vis.at[:, pl.ds(s * step_rows, step_rows)], ring.at[slot], ring_sem.at[slot])

    for s in range(slots - 1):
        fetch(s, s).start()

    def remote(src, dst, send, recv, device):
        return pltpu.make_async_remote_copy(
            src_ref=src, dst_ref=dst, send_sem=send, recv_sem=recv, device_id=device, device_id_type=MESH
        )

    out_at = lax.broadcasted_iota(jnp.int32, (SIDE, SIDE), 0)
    in_at = lax.broadcasted_iota(jnp.int32, (SIDE, SIDE), 1)
    one, nil = jnp.ones((), jnp.float32), jnp.zeros((), jnp.float32)
    spread[...] = jnp.where(in_at == lax.rem(out_at, kinds) * block + out_at // kinds, one, nil).astype(spread.dtype)
    gather[...] = jnp.where(in_at == lax.rem(out_at, block) * kinds + out_at // block, one, nil).astype(gather.dtype)
    table[blank] = jnp.zeros((kinds, LANES), table.dtype)
    spec_acc[...] = jnp.zeros(spec_acc.shape, spec_acc.dtype)

    flags = okay[...].astype(jnp.float32).astype(jnp.bfloat16)

    def look_up(first, seconds):
        n = first.shape[1]
        hot = jnp.where(lax.broadcasted_iota(jnp.int32, (dishes, n), 0) == first, one, nil).astype(jnp.bfloat16)
        rows = lax.dot_general(flags, hot, (((0,), (0,)), ((), ())), preferred_element_type=jnp.float32)
        at = lax.broadcasted_iota(jnp.int32, (cols, n), 0)
        good = None
        for second in seconds:
            hit = jnp.sum(jnp.where(at == second, rows, 0.0), 0, keepdims=True)
            good = hit if good is None else good * hit
        return good

    for level in range(levels):
        for i in range(packs):
            at = level * count + i * LANES
            a, b, c = [tri[pl.ds(e, 1), pl.ds(at, LANES)] for e in range(3)]
            second = b - jnp.bitwise_xor(me, 1 << level) * dishes
            row = second * cols + c
            if level == last:
                row = jnp.where(look_up(a - me * dishes, (b, c)) > 0.5, row, blank)
            asked[level, pl.ds(i, 1), :] = jnp.clip(row, 0, blank)

    def turn(s):
        slot = lax.rem(s, slots)
        fetch(s, slot).wait()
        for a in range(step_rows):
            for u in range(cols // (2 * block)):
                base = u * 2 * block
                x = jnp.concatenate(
                    [
                        jnp.concatenate(
                            [
                                ring[slot, plane, a, pl.ds(base + g * block, block), pl.ds(c * LANES, LANES)]
                                for c in range(chunks)
                                for plane in range(2)
                            ],
                            0,
                        )
                        for g in range(2)
                    ],
                    1,
                )
                y = dot(spread[...], x)
                for g in range(2):
                    rows = y[:, g * LANES : (g + 1) * LANES].reshape(block, kinds, LANES)
                    table[pl.ds((s * step_rows + a) * cols + base + g * block, block)] = rows.astype(table.dtype)

    def turn_step(s, _):
        @pl.when(s + slots - 1 < steps)
        def _():
            fetch(s + slots - 1, lax.rem(s + slots - 1, slots)).start()

        turn(s)
        return 0

    early, late = steps * 3 // 8, steps * 3 // 4
    lax.fori_loop(0, early, turn_step, 0)
    pl.semaphore_wait(barrier, len(peers) + len(others))
    ask = [
        remote(asked.at[level], got.at[level], idx_send.at[level], idx_recv.at[level], partner[level])
        for level in range(levels)
    ]
    for copy in ask:
        copy.start()
    lax.fori_loop(early, late, turn_step, 0)

    def slot_matrix(place):
        at = lax.broadcasted_iota(jnp.int32, (room, LANES), 0)
        for i in range(packs):
            mine = place[i : i + 1, :].astype(jnp.int32)
            hot[:, pl.ds(i * LANES, LANES)] = jnp.where(at == mine, one, nil).astype(hot.dtype)

    def by_slot(lists):
        parts = []
        for rows in lists:
            flat = blank - jnp.concatenate([rows[i : i + 1, :] for i in range(packs)], 1)
            parts += [flat // LANES, lax.rem(flat, LANES)]
        parts.append(jnp.zeros((8 - len(parts), count), jnp.int32))
        digits = jnp.concatenate(parts, 0).astype(jnp.float32).astype(jnp.bfloat16)
        moved = lax.dot_general(digits, hot[...], (((1,), (1,)), ((), ())), preferred_element_type=jnp.float32)
        out = []
        for i in range(len(lists)):
            value = moved[2 * i : 2 * i + 1] * LANES + moved[2 * i + 1 : 2 * i + 2]
            out.append(jnp.clip(blank - value.astype(jnp.int32), 0, blank))
        return out

    ask[last].wait()
    for i in range(packs):
        row = got[last, pl.ds(i, 1), :]
        good_out[last, pl.ds(i, 1), :] = look_up(row // cols, (lax.rem(row, cols),))
    good = good_out[last]
    low = lax.broadcasted_iota(jnp.int32, (LANES, LANES), 0)
    high = lax.broadcasted_iota(jnp.int32, (LANES, LANES), 1)
    before = dot(good.astype(jnp.bfloat16), jnp.where(low < high, one, nil).astype(jnp.bfloat16))
    each = dot(good.astype(jnp.bfloat16), jnp.ones((LANES, LANES), jnp.bfloat16))
    running, starts = jnp.zeros((1, LANES), jnp.float32), []
    for i in range(packs):
        starts.append(running)
        running = running + each[i : i + 1, :]
    place = jnp.where(good > 0.5, before + jnp.concatenate(starts, 0), float(2 * count))
    excess[...] = jnp.where(running > float(room), one, nil)
    good_out[last] = place
    slot_matrix(place)
    (rows,) = by_slot([got[last]])
    far_rows[...] = jnp.full(far_rows.shape, blank, far_rows.dtype)
    for i in range(room // LANES):
        far_rows[pl.ds(i, 1), :] = rows[:, i * LANES : (i + 1) * LANES]
    moves = []
    for level in reversed(range(levels)):
        if level < last:
            ask[level].wait()
        rows = far_rows if level == last else got.at[level]
        moves.append(pltpu.make_async_copy(rows, ask_smem.at[level], move_sem.at[level]))
        moves[-1].start()
    lax.fori_loop(late, steps, turn_step, 0)

    def take(level, start, n):
        unroll = 32

        def some(it, _):
            at = start + it * unroll
            pack, lane = at // LANES, lax.rem(at, LANES)
            for u in range(unroll):
                bc_send[level, at + u] = table[ask_smem[level, pack, lane + u]]
            return 0

        lax.fori_loop(0, n // unroll, some, 0)

    far = [
        remote(
            bc_send.at[last, pl.ds(k * FAR, FAR)],
            bc_recv.at[last, pl.ds(k * FAR, FAR)],
            far_send.at[k],
            far_recv.at[k],
            partner[last],
        )
        for k in range(pieces)
    ]
    near = [
        remote(bc_send.at[level], bc_recv.at[level], near_send.at[level], near_recv.at[level], partner[level])
        for level in range(last)
    ]
    send_good = [
        remote(good_out.at[level], good_in.at[level], good_send.at[level], good_recv.at[level], partner[level])
        for level in range(levels)
    ]

    def look_up_asked(level):
        for i in range(packs):
            row = got[level, pl.ds(i, 1), :]
            good_out[level, pl.ds(i, 1), :] = look_up(row // cols, (lax.rem(row, cols),))

    for move in moves:
        move.wait()
    take(last, 0, FAR)
    take(last, FAR, FAR)
    far[0].start()
    send_good[last].start()
    far[1].start()
    for k in range(2, pieces):
        take(last, k * FAR, FAR)
        if k > 2:
            far[k - 1].start()
    for level in range(last):
        look_up_asked(level)
        take(level, 0, count)
        if level == 0:
            far[pieces - 1].start()
        send_good[level].start()
    goods = []
    for level in range(last):
        for i in range(packs):
            at = level * count + i * LANES
            a, b, c = [tri[pl.ds(e, 1), pl.ds(at, LANES)] for e in range(3)]
            goods.append(look_up(a - me * dishes, (b, c)))
        near[level].start()
    for level in range(last):
        send_good[level].wait()
        for i in range(packs):
            at = level * count + i * LANES
            a, b, c = [tri[pl.ds(e, 1), pl.ds(at, LANES)] for e in range(3)]
            first = a - me * dishes
            good = goods[level * packs + i] * good_in[level, pl.ds(i, 1), :] > 0.5
            own_rows[level, 0, pl.ds(i, 1), :] = jnp.clip(jnp.where(good, first * cols + b, blank), 0, blank)
            own_rows[level, 1, pl.ds(i, 1), :] = jnp.clip(first * cols + c, 0, blank)
    send_good[last].wait()
    slot_matrix(good_in[last])
    lists = [[], []]
    for i in range(packs):
        at = last * count + i * LANES
        a, b, c = [tri[pl.ds(e, 1), pl.ds(at, LANES)] for e in range(3)]
        first = a - me * dishes
        lists[0].append(first * cols + b)
        lists[1].append(first * cols + c)
    for e, rows in enumerate(by_slot([jnp.concatenate(rows, 0) for rows in lists])):
        own_rows[last, e] = jnp.full((packs, LANES), blank, jnp.int32)
        for i in range(room // LANES):
            own_rows[last, e, pl.ds(i, 1), :] = rows[:, i * LANES : (i + 1) * LANES]
    move_own = pltpu.make_async_copy(own_rows, own_smem, move_sem.at[levels])
    move_own.start()
    move_own.wait()

    def products(level, n_blocks, n):
        def some(it, _):
            for s in range(n_blocks):
                start = (it * n_blocks + s) * block
                pack, lane = start // LANES, lax.rem(start, LANES)
                for u in range(block):
                    for e in range(2):
                        row = table[own_smem[level, e, pack, lane + u]]
                        pair[s, e, pl.ds(u * kinds, kinds), :] = row
            for s in range(n_blocks):
                start = pl.multiple_of((it * n_blocks + s) * block, block)
                y = dot(gather[...], jnp.concatenate([pair[s, 0], pair[s, 1]], 1))
                for c in range(chunks):
                    at = 2 * c * block
                    a_r, a_i = y[at : at + block, :LANES], y[at + block : at + 2 * block, :LANES]
                    c_r, c_i = y[at : at + block, LANES:], y[at + block : at + 2 * block, LANES:]
                    prod[level, 0, c, pl.ds(start, block), :] = a_r * c_r + a_i * c_i
                    prod[level, 1, c, pl.ds(start, block), :] = a_i * c_r - a_r * c_i
            return 0

        lax.fori_loop(0, n // (n_blocks * block), some, 0)

    def bispectra(level, start, n):
        wide = min(2, n // block)
        acc = [None] * (3 * chunks)
        for s in range(n // (wide * block)):
            begin = pl.multiple_of(start + s * wide * block, wide * block)
            x = [bc_recv[level, pl.ds(begin + g * block, block)].reshape(SIDE, LANES) for g in range(wide)]
            y = dot(gather[...], jnp.concatenate(x, 1) if wide > 1 else x[0])
            for g in range(wide):
                lanes = slice(g * LANES, (g + 1) * LANES)
                rows = pl.ds(begin + g * block, block)
                total_r = total_i = None
                for c in range(chunks):
                    at = 2 * c * block
                    b_r, b_i = y[at : at + block, lanes], y[at + block : at + 2 * block, lanes]
                    w_r, w_i = prod[level, 0, c, rows, :], prod[level, 1, c, rows, :]
                    real = w_r * b_r - w_i * b_i
                    imag = w_r * b_i + w_i * b_r
                    norm = jnp.sqrt(real * real + imag * imag)
                    for part, value in enumerate((real, imag, norm)):
                        value = fold(value)
                        old = acc[3 * c + part]
                        acc[3 * c + part] = value if old is None else old + value
                    total_r = real if c == 0 else total_r + real
                    total_i = imag if c == 0 else total_i + imag
                line[0, pl.ds(s * wide * block + g * block, block), :] = total_r
                line[1, pl.ds(s * wide * block + g * block, block), :] = total_i
        for c in range(chunks):
            for part in range(3):
                spec_acc[c, part] = spec_acc[c, part] + acc[3 * c + part]
        ones = jnp.ones((8, LANES), jnp.float32)
        for part in range(2):
            lane_sum = lax.dot_general(
                ones,
                line[part, pl.ds(0, n), :],
                (((1,), (1,)), ((), ())),
                precision=lax.Precision.HIGHEST,
                preferred_element_type=jnp.float32,
            )
            sums[0, level, pl.ds(part, 1), pl.ds(pl.multiple_of(start, LANES), n)] = lane_sum[:1]

    for level in range(levels):
        products(level, 4 * 32 // block, room if level == last else count)
    for level in range(last):
        near[level].wait()
        lax.fori_loop(0, count // 256, lambda it, _, level=level: (bispectra(level, it * 256, 256), 0)[1], 0)
    ahead = [
        remote(sums.at[0, level], sums.at[k, level], sum_send.at[k, level], sum_recv.at[k, level], device)
        for k, device in enumerate(peers, 1)
        for level in range(last)
    ]
    for k in range(pieces):
        far[k].wait()
        bispectra(last, k * FAR, FAR)
        if k == 0:
            for copy in ahead:
                copy.start()
    copies = list(ahead)
    for k, device in enumerate(peers, 1):
        whole = pl.ds(0, room)
        copies.append(
            remote(
                sums.at[0, last, :, whole],
                sums.at[k, last, :, whole],
                sum_send.at[k, last],
                sum_recv.at[k, last],
                device,
            )
        )
        copies[-1].start()
    for c in range(chunks):
        for part in range(3):
            spec_out[c, pl.ds(part, 1), :] = jnp.sum(spec_acc[c, part], 0, keepdims=True)
        spec_out[c, pl.ds(3, 1), :] = excess[...]
    spread_out = []
    for k, device in enumerate(others, 1):
        spread_out.append(
            remote(
                spec_out.at[device[1] * width // LANES],
                spec_recv.at[k],
                spec_send_sem.at[k],
                spec_recv_sem.at[k],
                device,
            )
        )
        spread_out[-1].start()
    for copy in copies:
        copy.wait()
    bands = channels * groups
    for level in range(levels):
        n = room if level == last else count
        total = sums[0, level, :, pl.ds(0, n)]
        for k in range(1, groups):
            total = total + sums[k, level, :, pl.ds(0, n)]
        total = total / bands
        if level == last:
            parts, rest = [], total
            for _ in range(3):
                parts.append(rest.astype(jnp.bfloat16).astype(jnp.float32))
                rest = rest - parts[-1]
            parts.append(jnp.zeros((2, room), jnp.float32))
            moved = dot(jnp.concatenate(parts, 0).astype(jnp.bfloat16), hot[...])
            total = moved[0:2] + moved[2:4] + moved[4:6]
        means[:, pl.ds(level * count, count)] = total
    for copy in spread_out:
        copy.wait()
    total = spec_out[me * width // LANES]
    for k in range(1, tiles):
        total = total + spec_recv[k]
    closure[pl.ds(0, 2), :] = total[:2] / (1.0 + total[2:3])
    closure[pl.ds(2, 1), :] = total[3:4]


def body(visibility, dish_pair_okay, triangles):
    _, dishes, cols, channels = visibility.shape
    levels = triangles.shape[1] // TRI_LVL
    tiles, groups = lax.axis_size("tile"), lax.axis_size("grp")
    chunks = channels // LANES
    kinds = 2 * chunks
    packs = TRI_LVL // LANES
    step_rows, slots = 4, 3
    room = far_room(TRI_LVL)
    pieces = room // FAR
    width = channels // tiles
    vmem = pl.BlockSpec(memory_space=pltpu.VMEM)
    f32, bf16, i32 = jnp.float32, jnp.bfloat16, jnp.int32
    dma = pltpu.SemaphoreType.DMA
    triangle_means, closure = pl.pallas_call(
        functools.partial(mega_kernel, groups=groups, tiles=tiles, levels=levels, step_rows=step_rows),
        in_specs=[pl.BlockSpec(memory_space=pl.ANY), vmem, vmem],
        out_specs=[vmem, vmem],
        out_shape=[
            jax.ShapeDtypeStruct((2, triangles.shape[1]), f32),
            jax.ShapeDtypeStruct((3, LANES), f32),
        ],
        scratch_shapes=[
            pltpu.VMEM((dishes * cols + 1, kinds, LANES), bf16),
            pltpu.VMEM((slots, 2, step_rows, cols, channels), bf16),
            pltpu.VMEM((SIDE, SIDE), bf16),
            pltpu.VMEM((SIDE, SIDE), bf16),
            pltpu.VMEM((levels, packs, LANES), i32),
            pltpu.VMEM((levels, packs, LANES), i32),
            pltpu.VMEM((levels, packs, LANES), f32),
            pltpu.VMEM((levels, packs, LANES), f32),
            pltpu.VMEM((packs, LANES), i32),
            pltpu.VMEM((room, TRI_LVL), bf16),
            pltpu.VMEM((1, LANES), f32),
            pltpu.VMEM((levels, 2, packs, LANES), i32),
            pltpu.SMEM((levels, packs, LANES), i32),
            pltpu.SMEM((levels, 2, packs, LANES), i32),
            pltpu.VMEM((levels, TRI_LVL, kinds, LANES), bf16),
            pltpu.VMEM((levels, TRI_LVL, kinds, LANES), bf16),
            pltpu.VMEM((4, 2, SIDE, LANES), bf16),
            pltpu.VMEM((levels, 2, chunks, TRI_LVL, LANES), f32),
            pltpu.VMEM((2, 256, LANES), f32),
            pltpu.VMEM((groups, levels, 2, TRI_LVL), f32),
            pltpu.VMEM((chunks, 3, 8, LANES), f32),
            pltpu.VMEM((chunks, 8, LANES), f32),
            pltpu.VMEM((tiles, 8, LANES), f32),
            dma((slots,)),
            dma((levels + 1,)),
            dma((levels,)),
            dma((levels,)),
            dma((levels,)),
            dma((levels,)),
            dma((levels,)),
            dma((levels,)),
            dma((pieces,)),
            dma((pieces,)),
            dma((groups, levels)),
            dma((groups, levels)),
            dma((tiles,)),
            dma((tiles,)),
        ],
        compiler_params=pltpu.CompilerParams(
            collective_id=0, has_side_effects=True, vmem_limit_bytes=67043328
        ),
        name="bispectra",
    )(visibility, dish_pair_okay, triangles)
    at = lax.rem(lax.axis_index("tile") * width, LANES)
    return lax.cond(
        closure[2, 0] > 0.5,
        lambda: every_row(visibility, dish_pair_okay, triangles),
        lambda: (triangle_means, lax.dynamic_slice(closure, (0, at), (2, width))),
    )


def every_row(visibility, dish_pair_okay, triangles):
    _, dishes, cols, channels = visibility.shape
    levels = triangles.shape[1] // TRI_LVL
    tiles, groups = lax.axis_size("tile"), lax.axis_size("grp")
    device = lax.axis_index("tile")
    table = visibility.reshape(2, dishes * cols, channels)
    flags = dish_pair_okay.reshape(-1).astype(jnp.float32)
    means, spectrum = [], 0.0
    for level in range(levels):
        pairs = [(i, i ^ 1 << level) for i in range(tiles)]
        a, b, c = triangles[:, level * TRI_LVL : (level + 1) * TRI_LVL]
        first = (a - device * dishes) * cols
        asked = (b - jnp.bitwise_xor(device, 1 << level) * dishes) * cols + c
        asked = lax.ppermute(asked, "tile", pairs)
        bc = lax.ppermute(table[:, asked], "tile", pairs).astype(jnp.float32)
        weight = lax.ppermute(flags[asked], "tile", pairs) * flags[first + b] * flags[first + c]
        ab, ac = [table[:, first + x].astype(jnp.float32) for x in (b, c)]
        p_r, p_i = ab[0] * bc[0] - ab[1] * bc[1], ab[0] * bc[1] + ab[1] * bc[0]
        real = weight[:, None] * (p_r * ac[0] + p_i * ac[1])
        imag = weight[:, None] * (p_i * ac[0] - p_r * ac[1])
        norm = jnp.sqrt(real * real + imag * imag)
        spectrum = spectrum + jnp.stack([x.sum(0) for x in (real, imag, norm)])
        means.append(jnp.stack([x.sum(1) for x in (real, imag)]))
    means = lax.psum(jnp.concatenate(means, 1), "grp") / (channels * groups)
    spectrum = lax.psum(spectrum, "tile")
    closure = spectrum[:2] / (1.0 + spectrum[2])
    width = channels // tiles
    return means, lax.dynamic_slice_in_dim(closure, device * width, width, 1)


def solution(mesh):
    return jax.shard_map(
        body,
        mesh=mesh,
        in_specs=(P(None, "tile", None, "grp"), P("tile", None), P(None, "tile")),
        out_specs=(P(None, "tile"), P(None, ("grp", "tile"))),
        check_vma=False,
    )
```

```python
import functools

import jax
import jax.numpy as jnp
from jax import lax
from jax.experimental import pallas as pl
from jax.experimental.pallas import tpu as pltpu
from jax.sharding import PartitionSpec as P

TRI_LVL = 1024
LANES = 128
SIDE = 256
FAR = 128
FIRST = 256
EARLY = 1
MESH = pl.DeviceIdType.MESH


def dot(a, b):
    return lax.dot_general(a, b, (((1,), (0,)), ((), ())), preferred_element_type=jnp.float32)


def fold(x):
    total = x[:8]
    for i in range(1, x.shape[0] // 8):
        total = total + x[i * 8 : i * 8 + 8]
    return total


def far_room(count):
    return count * 3 // 4 // FAR * FAR


def mega_kernel(
    vis,
    okay,
    tri,
    means,
    closure,
    table,
    ring,
    spread,
    gather,
    asked,
    got,
    good_out,
    good_in,
    far_rows,
    hot,
    excess,
    own_rows,
    ask_smem,
    own_smem,
    bc_send,
    bc_recv,
    pair,
    prod,
    line,
    sums,
    spec_acc,
    spec_out,
    spec_recv,
    ring_sem,
    move_sem,
    idx_send,
    idx_recv,
    good_send,
    good_recv,
    near_send,
    near_recv,
    far_send,
    far_recv,
    sum_send,
    sum_recv,
    spec_send_sem,
    spec_recv_sem,
    *,
    groups,
    tiles,
    levels,
    step_rows,
):
    _, dishes, cols, channels = vis.shape
    chunks = channels // LANES
    kinds = 2 * chunks
    block = SIDE // kinds
    blank = dishes * cols
    count = tri.shape[1] // levels
    packs = count // LANES
    last = levels - 1
    slots = ring.shape[0]
    steps = dishes // step_rows
    room = far_room(count)
    pieces = room // FAR
    width = channels // tiles
    me_g, me = lax.axis_index("grp"), lax.axis_index("tile")
    peers = [(lax.rem(me_g + k, groups), me) for k in range(1, groups)]
    others = [(me_g, lax.rem(me + k, tiles)) for k in range(1, tiles)]
    partner = [(me_g, jnp.bitwise_xor(me, 1 << level)) for level in range(levels)]

    barrier = pltpu.get_barrier_semaphore()
    for device in peers + others:
        pl.semaphore_signal(barrier, inc=1, device_id=device, device_id_type=MESH)

    def fetch(s, slot):
        return pltpu.make_async_copy(vis.at[:, pl.ds(s * step_rows, step_rows)], ring.at[slot], ring_sem.at[slot])

    for s in range(slots - 1):
        fetch(s, s).start()

    def remote(src, dst, send, recv, device):
        return pltpu.make_async_remote_copy(
            src_ref=src, dst_ref=dst, send_sem=send, recv_sem=recv, device_id=device, device_id_type=MESH
        )

    out_at = lax.broadcasted_iota(jnp.int32, (SIDE, SIDE), 0)
    in_at = lax.broadcasted_iota(jnp.int32, (SIDE, SIDE), 1)
    one, nil = jnp.ones((), jnp.float32), jnp.zeros((), jnp.float32)
    spread[...] = jnp.where(in_at == lax.rem(out_at, kinds) * block + out_at // kinds, one, nil).astype(spread.dtype)
    gather[...] = jnp.where(in_at == lax.rem(out_at, block) * kinds + out_at // block, one, nil).astype(gather.dtype)
    table[blank] = jnp.zeros((kinds, LANES), table.dtype)
    spec_acc[...] = jnp.zeros(spec_acc.shape, spec_acc.dtype)

    flags = okay[...].astype(jnp.float32).astype(jnp.bfloat16)

    def look_up(first, seconds):
        n = first.shape[1]
        hot = jnp.where(lax.broadcasted_iota(jnp.int32, (dishes, n), 0) == first, one, nil).astype(jnp.bfloat16)
        rows = lax.dot_general(flags, hot, (((0,), (0,)), ((), ())), preferred_element_type=jnp.float32)
        at = lax.broadcasted_iota(jnp.int32, (cols, n), 0)
        good = None
        for second in seconds:
            hit = jnp.sum(jnp.where(at == second, rows, 0.0), 0, keepdims=True)
            good = hit if good is None else good * hit
        return good

    for level in range(levels):
        for i in range(packs):
            at = level * count + i * LANES
            a, b, c = [tri[pl.ds(e, 1), pl.ds(at, LANES)] for e in range(3)]
            second = b - jnp.bitwise_xor(me, 1 << level) * dishes
            row = second * cols + c
            if level == last:
                row = jnp.where(look_up(a - me * dishes, (b, c)) > 0.5, row, blank)
            asked[level, pl.ds(i, 1), :] = jnp.clip(row, 0, blank)

    def turn(s):
        slot = lax.rem(s, slots)
        fetch(s, slot).wait()
        for a in range(step_rows):
            for u in range(cols // (2 * block)):
                base = u * 2 * block
                x = jnp.concatenate(
                    [
                        jnp.concatenate(
                            [
                                ring[slot, plane, a, pl.ds(base + g * block, block), pl.ds(c * LANES, LANES)]
                                for c in range(chunks)
                                for plane in range(2)
                            ],
                            0,
                        )
                        for g in range(2)
                    ],
                    1,
                )
                y = dot(spread[...], x)
                for g in range(2):
                    rows = y[:, g * LANES : (g + 1) * LANES].reshape(block, kinds, LANES)
                    table[pl.ds((s * step_rows + a) * cols + base + g * block, block)] = rows.astype(table.dtype)

    def turn_step(s, _):
        @pl.when(s + slots - 1 < steps)
        def _():
            fetch(s + slots - 1, lax.rem(s + slots - 1, slots)).start()

        turn(s)
        return 0

    early, late, ready = EARLY, max(EARLY, steps * 3 // 8), steps // 2
    lax.fori_loop(0, early, turn_step, 0)
    pl.semaphore_wait(barrier, len(peers) + len(others))
    ask = [
        remote(asked.at[level], got.at[level], idx_send.at[level], idx_recv.at[level], partner[level])
        for level in range(levels)
    ]
    for copy in ask:
        copy.start()
    lax.fori_loop(early, late, turn_step, 0)

    def slot_matrix(place):
        at = lax.broadcasted_iota(jnp.int32, (room, LANES), 0)
        for i in range(packs):
            mine = place[i : i + 1, :].astype(jnp.int32)
            hot[:, pl.ds(i * LANES, LANES)] = jnp.where(at == mine, one, nil).astype(hot.dtype)

    def by_slot(lists):
        parts = []
        for rows in lists:
            flat = blank - jnp.concatenate([rows[i : i + 1, :] for i in range(packs)], 1)
            parts += [flat // LANES, lax.rem(flat, LANES)]
        parts.append(jnp.zeros((8 - len(parts), count), jnp.int32))
        digits = jnp.concatenate(parts, 0).astype(jnp.float32).astype(jnp.bfloat16)
        moved = lax.dot_general(digits, hot[...], (((1,), (1,)), ((), ())), preferred_element_type=jnp.float32)
        out = []
        for i in range(len(lists)):
            value = moved[2 * i : 2 * i + 1] * LANES + moved[2 * i + 1 : 2 * i + 2]
            out.append(jnp.clip(blank - value.astype(jnp.int32), 0, blank))
        return out

    ask[last].wait()
    for i in range(packs):
        row = got[last, pl.ds(i, 1), :]
        good_out[last, pl.ds(i, 1), :] = look_up(row // cols, (lax.rem(row, cols),))
    good = good_out[last]
    antenna = got[last] // cols
    low = lax.broadcasted_iota(jnp.int32, (LANES, LANES), 0)
    high = lax.broadcasted_iota(jnp.int32, (LANES, LANES), 1)
    ahead_of = jnp.where(low < high, one, nil).astype(jnp.bfloat16)
    every = jnp.ones((LANES, LANES), jnp.bfloat16)
    number = lax.broadcasted_iota(jnp.int32, (dishes, LANES), 0)
    running, seen = jnp.zeros((dishes, LANES), jnp.float32), []
    for i in range(packs):
        mine = jnp.where(number == antenna[i : i + 1, :], good[i : i + 1, :], 0.0)
        mark = mine.astype(jnp.bfloat16)
        seen.append((mine, running + dot(mark, ahead_of)))
        running = running + dot(mark, every)
    row = lax.broadcasted_iota(jnp.int32, (dishes, dishes), 0)
    column = lax.broadcasted_iota(jnp.int32, (dishes, dishes), 1)
    offset = lax.dot_general(
        jnp.where(column < row, one, nil),
        running,
        (((1,), (0,)), ((), ())),
        precision=lax.Precision.HIGHEST,
        preferred_element_type=jnp.float32,
    )
    place = jnp.concatenate([jnp.sum(mine * (at + offset), 0, keepdims=True) for mine, at in seen], 0)
    place = jnp.where(good > 0.5, place, float(2 * count))
    used = jnp.sum(running, 0, keepdims=True)
    soon = jnp.sum(jnp.where(number < ready * step_rows, running, 0.0), 0, keepdims=True)
    fits = (used <= float(room)) & (soon >= jnp.minimum(used, float(FIRST)))
    excess[...] = jnp.where(fits, nil, one)
    good_out[last] = place
    slot_matrix(place)
    (rows,) = by_slot([got[last]])
    far_rows[...] = jnp.full(far_rows.shape, blank, far_rows.dtype)
    for i in range(room // LANES):
        far_rows[pl.ds(i, 1), :] = rows[:, i * LANES : (i + 1) * LANES]
    moves = []
    for level in reversed(range(levels)):
        if level < last:
            ask[level].wait()
        rows = far_rows if level == last else got.at[level]
        moves.append(pltpu.make_async_copy(rows, ask_smem.at[level], move_sem.at[level]))
        moves[-1].start()
    lax.fori_loop(late, ready, turn_step, 0)

    def take(level, start, n):
        unroll = 32

        def some(it, _):
            at = start + it * unroll
            pack, lane = at // LANES, lax.rem(at, LANES)
            for u in range(unroll):
                bc_send[level, at + u] = table[ask_smem[level, pack, lane + u]]
            return 0

        lax.fori_loop(0, n // unroll, some, 0)

    far = [
        remote(
            bc_send.at[last, pl.ds(k * FAR, FAR)],
            bc_recv.at[last, pl.ds(k * FAR, FAR)],
            far_send.at[k],
            far_recv.at[k],
            partner[last],
        )
        for k in range(pieces)
    ]
    near = [
        remote(bc_send.at[level], bc_recv.at[level], near_send.at[level], near_recv.at[level], partner[level])
        for level in range(last)
    ]
    send_good = [
        remote(good_out.at[level], good_in.at[level], good_send.at[level], good_recv.at[level], partner[level])
        for level in range(levels)
    ]

    def look_up_asked(level):
        for i in range(packs):
            row = got[level, pl.ds(i, 1), :]
            good_out[level, pl.ds(i, 1), :] = look_up(row // cols, (lax.rem(row, cols),))

    for move in moves:
        move.wait()
    for k in range(FIRST // FAR):
        take(last, k * FAR, FAR)
    for k in range(FIRST // FAR):
        far[k].start()
        if k == 0:
            send_good[last].start()
    lax.fori_loop(ready, steps, turn_step, 0)
    for k in range(FIRST // FAR, pieces):
        take(last, k * FAR, FAR)
        if k > FIRST // FAR:
            far[k - 1].start()
    for level in range(last):
        look_up_asked(level)
        take(level, 0, count)
        if level == 0:
            far[pieces - 1].start()
        send_good[level].start()
    goods = []
    for level in range(last):
        for i in range(packs):
            at = level * count + i * LANES
            a, b, c = [tri[pl.ds(e, 1), pl.ds(at, LANES)] for e in range(3)]
            goods.append(look_up(a - me * dishes, (b, c)))
        near[level].start()
    for level in range(last):
        send_good[level].wait()
        for i in range(packs):
            at = level * count + i * LANES
            a, b, c = [tri[pl.ds(e, 1), pl.ds(at, LANES)] for e in range(3)]
            first = a - me * dishes
            good = goods[level * packs + i] * good_in[level, pl.ds(i, 1), :] > 0.5
            own_rows[level, 0, pl.ds(i, 1), :] = jnp.clip(jnp.where(good, first * cols + b, blank), 0, blank)
            own_rows[level, 1, pl.ds(i, 1), :] = jnp.clip(first * cols + c, 0, blank)
    send_good[last].wait()
    slot_matrix(good_in[last])
    lists = [[], []]
    for i in range(packs):
        at = last * count + i * LANES
        a, b, c = [tri[pl.ds(e, 1), pl.ds(at, LANES)] for e in range(3)]
        first = a - me * dishes
        lists[0].append(first * cols + b)
        lists[1].append(first * cols + c)
    for e, rows in enumerate(by_slot([jnp.concatenate(rows, 0) for rows in lists])):
        own_rows[last, e] = jnp.full((packs, LANES), blank, jnp.int32)
        for i in range(room // LANES):
            own_rows[last, e, pl.ds(i, 1), :] = rows[:, i * LANES : (i + 1) * LANES]
    move_own = pltpu.make_async_copy(own_rows, own_smem, move_sem.at[levels])
    move_own.start()
    move_own.wait()

    def products(level, n_blocks, n):
        def some(it, _):
            for s in range(n_blocks):
                start = (it * n_blocks + s) * block
                pack, lane = start // LANES, lax.rem(start, LANES)
                for u in range(block):
                    for e in range(2):
                        row = table[own_smem[level, e, pack, lane + u]]
                        pair[s, e, pl.ds(u * kinds, kinds), :] = row
            for s in range(n_blocks):
                start = pl.multiple_of((it * n_blocks + s) * block, block)
                y = dot(gather[...], jnp.concatenate([pair[s, 0], pair[s, 1]], 1))
                for c in range(chunks):
                    at = 2 * c * block
                    a_r, a_i = y[at : at + block, :LANES], y[at + block : at + 2 * block, :LANES]
                    c_r, c_i = y[at : at + block, LANES:], y[at + block : at + 2 * block, LANES:]
                    prod[level, 0, c, pl.ds(start, block), :] = a_r * c_r + a_i * c_i
                    prod[level, 1, c, pl.ds(start, block), :] = a_i * c_r - a_r * c_i
            return 0

        lax.fori_loop(0, n // (n_blocks * block), some, 0)

    def bispectra(level, start, n):
        wide = min(2, n // block)
        acc = [None] * (3 * chunks)
        for s in range(n // (wide * block)):
            begin = pl.multiple_of(start + s * wide * block, wide * block)
            x = [bc_recv[level, pl.ds(begin + g * block, block)].reshape(SIDE, LANES) for g in range(wide)]
            y = dot(gather[...], jnp.concatenate(x, 1) if wide > 1 else x[0])
            for g in range(wide):
                lanes = slice(g * LANES, (g + 1) * LANES)
                rows = pl.ds(begin + g * block, block)
                total_r = total_i = None
                for c in range(chunks):
                    at = 2 * c * block
                    b_r, b_i = y[at : at + block, lanes], y[at + block : at + 2 * block, lanes]
                    w_r, w_i = prod[level, 0, c, rows, :], prod[level, 1, c, rows, :]
                    real = w_r * b_r - w_i * b_i
                    imag = w_r * b_i + w_i * b_r
                    norm = jnp.sqrt(real * real + imag * imag)
                    for part, value in enumerate((real, imag, norm)):
                        value = fold(value)
                        old = acc[3 * c + part]
                        acc[3 * c + part] = value if old is None else old + value
                    total_r = real if c == 0 else total_r + real
                    total_i = imag if c == 0 else total_i + imag
                line[0, pl.ds(s * wide * block + g * block, block), :] = total_r
                line[1, pl.ds(s * wide * block + g * block, block), :] = total_i
        for c in range(chunks):
            for part in range(3):
                spec_acc[c, part] = spec_acc[c, part] + acc[3 * c + part]
        ones = jnp.ones((8, LANES), jnp.float32)
        for part in range(2):
            lane_sum = lax.dot_general(
                ones,
                line[part, pl.ds(0, n), :],
                (((1,), (1,)), ((), ())),
                precision=lax.Precision.HIGHEST,
                preferred_element_type=jnp.float32,
            )
            sums[0, level, pl.ds(part, 1), pl.ds(pl.multiple_of(start, LANES), n)] = lane_sum[:1]

    for level in range(levels):
        products(level, 4 * 32 // block, room if level == last else count)
    for level in range(last):
        near[level].wait()
        lax.fori_loop(0, count // 256, lambda it, _, level=level: (bispectra(level, it * 256, 256), 0)[1], 0)
    ahead = [
        remote(sums.at[0, level], sums.at[k, level], sum_send.at[k, level], sum_recv.at[k, level], device)
        for k, device in enumerate(peers, 1)
        for level in range(last)
    ]
    for k in range(pieces):
        far[k].wait()
        bispectra(last, k * FAR, FAR)
        if k == 0:
            for copy in ahead:
                copy.start()
    copies = list(ahead)
    for k, device in enumerate(peers, 1):
        whole = pl.ds(0, room)
        copies.append(
            remote(
                sums.at[0, last, :, whole],
                sums.at[k, last, :, whole],
                sum_send.at[k, last],
                sum_recv.at[k, last],
                device,
            )
        )
        copies[-1].start()
    for c in range(chunks):
        for part in range(3):
            spec_out[c, pl.ds(part, 1), :] = jnp.sum(spec_acc[c, part], 0, keepdims=True)
        spec_out[c, pl.ds(3, 1), :] = excess[...]
    spread_out = []
    for k, device in enumerate(others, 1):
        spread_out.append(
            remote(
                spec_out.at[device[1] * width // LANES],
                spec_recv.at[k],
                spec_send_sem.at[k],
                spec_recv_sem.at[k],
                device,
            )
        )
        spread_out[-1].start()
    for copy in copies:
        copy.wait()
    bands = channels * groups
    for level in range(levels):
        n = room if level == last else count
        total = sums[0, level, :, pl.ds(0, n)]
        for k in range(1, groups):
            total = total + sums[k, level, :, pl.ds(0, n)]
        total = total / bands
        if level == last:
            parts, rest = [], total
            for _ in range(3):
                parts.append(rest.astype(jnp.bfloat16).astype(jnp.float32))
                rest = rest - parts[-1]
            parts.append(jnp.zeros((2, room), jnp.float32))
            moved = dot(jnp.concatenate(parts, 0).astype(jnp.bfloat16), hot[...])
            total = moved[0:2] + moved[2:4] + moved[4:6]
        means[:, pl.ds(level * count, count)] = total
    for copy in spread_out:
        copy.wait()
    total = spec_out[me * width // LANES]
    for k in range(1, tiles):
        total = total + spec_recv[k]
    closure[pl.ds(0, 2), :] = total[:2] / (1.0 + total[2:3])
    closure[pl.ds(2, 1), :] = total[3:4]


def body(visibility, dish_pair_okay, triangles):
    _, dishes, cols, channels = visibility.shape
    levels = triangles.shape[1] // TRI_LVL
    tiles, groups = lax.axis_size("tile"), lax.axis_size("grp")
    chunks = channels // LANES
    kinds = 2 * chunks
    packs = TRI_LVL // LANES
    step_rows, slots = 4, 3
    room = far_room(TRI_LVL)
    pieces = room // FAR
    width = channels // tiles
    vmem = pl.BlockSpec(memory_space=pltpu.VMEM)
    f32, bf16, i32 = jnp.float32, jnp.bfloat16, jnp.int32
    dma = pltpu.SemaphoreType.DMA
    triangle_means, closure = pl.pallas_call(
        functools.partial(mega_kernel, groups=groups, tiles=tiles, levels=levels, step_rows=step_rows),
        in_specs=[pl.BlockSpec(memory_space=pl.ANY), vmem, vmem],
        out_specs=[vmem, vmem],
        out_shape=[
            jax.ShapeDtypeStruct((2, triangles.shape[1]), f32),
            jax.ShapeDtypeStruct((3, LANES), f32),
        ],
        scratch_shapes=[
            pltpu.VMEM((dishes * cols + 1, kinds, LANES), bf16),
            pltpu.VMEM((slots, 2, step_rows, cols, channels), bf16),
            pltpu.VMEM((SIDE, SIDE), bf16),
            pltpu.VMEM((SIDE, SIDE), bf16),
            pltpu.VMEM((levels, packs, LANES), i32),
            pltpu.VMEM((levels, packs, LANES), i32),
            pltpu.VMEM((levels, packs, LANES), f32),
            pltpu.VMEM((levels, packs, LANES), f32),
            pltpu.VMEM((packs, LANES), i32),
            pltpu.VMEM((room, TRI_LVL), bf16),
            pltpu.VMEM((1, LANES), f32),
            pltpu.VMEM((levels, 2, packs, LANES), i32),
            pltpu.SMEM((levels, packs, LANES), i32),
            pltpu.SMEM((levels, 2, packs, LANES), i32),
            pltpu.VMEM((levels, TRI_LVL, kinds, LANES), bf16),
            pltpu.VMEM((levels, TRI_LVL, kinds, LANES), bf16),
            pltpu.VMEM((4, 2, SIDE, LANES), bf16),
            pltpu.VMEM((levels, 2, chunks, TRI_LVL, LANES), f32),
            pltpu.VMEM((2, 256, LANES), f32),
            pltpu.VMEM((groups, levels, 2, TRI_LVL), f32),
            pltpu.VMEM((chunks, 3, 8, LANES), f32),
            pltpu.VMEM((chunks, 8, LANES), f32),
            pltpu.VMEM((tiles, 8, LANES), f32),
            dma((slots,)),
            dma((levels + 1,)),
            dma((levels,)),
            dma((levels,)),
            dma((levels,)),
            dma((levels,)),
            dma((levels,)),
            dma((levels,)),
            dma((pieces,)),
            dma((pieces,)),
            dma((groups, levels)),
            dma((groups, levels)),
            dma((tiles,)),
            dma((tiles,)),
        ],
        compiler_params=pltpu.CompilerParams(
            collective_id=0, has_side_effects=True, vmem_limit_bytes=67043328
        ),
        name="bispectra",
    )(visibility, dish_pair_okay, triangles)
    at = lax.rem(lax.axis_index("tile") * width, LANES)
    return lax.cond(
        closure[2, 0] > 0.5,
        lambda: every_row(visibility, dish_pair_okay, triangles),
        lambda: (triangle_means, lax.dynamic_slice(closure, (0, at), (2, width))),
    )


def every_row(visibility, dish_pair_okay, triangles):
    _, dishes, cols, channels = visibility.shape
    levels = triangles.shape[1] // TRI_LVL
    tiles, groups = lax.axis_size("tile"), lax.axis_size("grp")
    device = lax.axis_index("tile")
    table = visibility.reshape(2, dishes * cols, channels)
    flags = dish_pair_okay.reshape(-1).astype(jnp.float32)
    means, spectrum = [], 0.0
    for level in range(levels):
        pairs = [(i, i ^ 1 << level) for i in range(tiles)]
        a, b, c = triangles[:, level * TRI_LVL : (level + 1) * TRI_LVL]
        first = (a - device * dishes) * cols
        asked = (b - jnp.bitwise_xor(device, 1 << level) * dishes) * cols + c
        asked = lax.ppermute(asked, "tile", pairs)
        bc = lax.ppermute(table[:, asked], "tile", pairs).astype(jnp.float32)
        weight = lax.ppermute(flags[asked], "tile", pairs) * flags[first + b] * flags[first + c]
        ab, ac = [table[:, first + x].astype(jnp.float32) for x in (b, c)]
        p_r, p_i = ab[0] * bc[0] - ab[1] * bc[1], ab[0] * bc[1] + ab[1] * bc[0]
        real = weight[:, None] * (p_r * ac[0] + p_i * ac[1])
        imag = weight[:, None] * (p_i * ac[0] - p_r * ac[1])
        norm = jnp.sqrt(real * real + imag * imag)
        spectrum = spectrum + jnp.stack([x.sum(0) for x in (real, imag, norm)])
        means.append(jnp.stack([x.sum(1) for x in (real, imag)]))
    means = lax.psum(jnp.concatenate(means, 1), "grp") / (channels * groups)
    spectrum = lax.psum(spectrum, "tile")
    closure = spectrum[:2] / (1.0 + spectrum[2])
    width = channels // tiles
    return means, lax.dynamic_slice_in_dim(closure, device * width, width, 1)


def solution(mesh):
    return jax.shard_map(
        body,
        mesh=mesh,
        in_specs=(P(None, "tile", None, "grp"), P("tile", None), P(None, "tile")),
        out_specs=(P(None, "tile"), P(None, ("grp", "tile"))),
        check_vma=False,
    )
```

```python
import functools

import jax
import jax.numpy as jnp
from jax import lax
from jax.experimental import pallas as pl
from jax.experimental.pallas import tpu as pltpu
from jax.sharding import PartitionSpec as P

TRI_LVL = 1024
LANES = 128
SIDE = 256
FAR = 128
FIRST = 256
EARLY = 1
MESH = pl.DeviceIdType.MESH


def dot(a, b):
    return lax.dot_general(a, b, (((1,), (0,)), ((), ())), preferred_element_type=jnp.float32)


def fold(x):
    total = x[:8]
    for i in range(1, x.shape[0] // 8):
        total = total + x[i * 8 : i * 8 + 8]
    return total


def far_room(count):
    return count * 3 // 4 // FAR * FAR


def mega_kernel(
    vis,
    okay,
    tri,
    means,
    closure,
    missed,
    table,
    ring,
    spread,
    gather,
    asked,
    got,
    good_out,
    good_in,
    far_rows,
    hot,
    excess,
    own_rows,
    ask_smem,
    own_smem,
    bc_send,
    bc_recv,
    pair,
    prod,
    line,
    sums,
    spec_acc,
    spec_out,
    spec_recv,
    ring_sem,
    move_sem,
    idx_send,
    idx_recv,
    good_send,
    good_recv,
    near_send,
    near_recv,
    far_send,
    far_recv,
    sum_send,
    sum_recv,
    spec_send_sem,
    spec_recv_sem,
    *,
    groups,
    tiles,
    levels,
    step_rows,
):
    _, dishes, cols, channels = vis.shape
    chunks = channels // LANES
    kinds = 2 * chunks
    block = SIDE // kinds
    blank = dishes * cols
    count = tri.shape[1] // levels
    packs = count // LANES
    last = levels - 1
    slots = ring.shape[0]
    steps = dishes // step_rows
    room = far_room(count)
    pieces = room // FAR
    width = channels // tiles
    me_g, me = lax.axis_index("grp"), lax.axis_index("tile")
    peers = [(lax.rem(me_g + k, groups), me) for k in range(1, groups)]
    others = [(me_g, lax.rem(me + k, tiles)) for k in range(1, tiles)]
    partner = [(me_g, jnp.bitwise_xor(me, 1 << level)) for level in range(levels)]

    barrier = pltpu.get_barrier_semaphore()
    for device in peers + others:
        pl.semaphore_signal(barrier, inc=1, device_id=device, device_id_type=MESH)

    def fetch(s, slot):
        return pltpu.make_async_copy(vis.at[:, pl.ds(s * step_rows, step_rows)], ring.at[slot], ring_sem.at[slot])

    for s in range(slots - 1):
        fetch(s, s).start()

    def remote(src, dst, send, recv, device):
        return pltpu.make_async_remote_copy(
            src_ref=src, dst_ref=dst, send_sem=send, recv_sem=recv, device_id=device, device_id_type=MESH
        )

    out_at = lax.broadcasted_iota(jnp.int32, (SIDE, SIDE), 0)
    in_at = lax.broadcasted_iota(jnp.int32, (SIDE, SIDE), 1)
    one, nil = jnp.ones((), jnp.float32), jnp.zeros((), jnp.float32)
    spread[...] = jnp.where(in_at == lax.rem(out_at, kinds) * block + out_at // kinds, one, nil).astype(spread.dtype)
    gather[...] = jnp.where(in_at == lax.rem(out_at, block) * kinds + out_at // block, one, nil).astype(gather.dtype)
    table[blank] = jnp.zeros((kinds, LANES), table.dtype)
    spec_acc[...] = jnp.zeros(spec_acc.shape, spec_acc.dtype)

    flags = okay[...].astype(jnp.float32).astype(jnp.bfloat16)

    def look_up(first, seconds):
        n = first.shape[1]
        hot = jnp.where(lax.broadcasted_iota(jnp.int32, (dishes, n), 0) == first, one, nil).astype(jnp.bfloat16)
        rows = lax.dot_general(flags, hot, (((0,), (0,)), ((), ())), preferred_element_type=jnp.float32)
        at = lax.broadcasted_iota(jnp.int32, (cols, n), 0)
        good = None
        for second in seconds:
            hit = jnp.sum(jnp.where(at == second, rows, 0.0), 0, keepdims=True)
            good = hit if good is None else good * hit
        return good

    for level in range(levels):
        for i in range(packs):
            at = level * count + i * LANES
            a, b, c = [tri[pl.ds(e, 1), pl.ds(at, LANES)] for e in range(3)]
            second = b - jnp.bitwise_xor(me, 1 << level) * dishes
            row = second * cols + c
            if level == last:
                row = jnp.where(look_up(a - me * dishes, (b, c)) > 0.5, row, blank)
            asked[level, pl.ds(i, 1), :] = jnp.clip(row, 0, blank)

    def turn(s):
        slot = lax.rem(s, slots)
        fetch(s, slot).wait()
        for a in range(step_rows):
            for u in range(cols // (2 * block)):
                base = u * 2 * block
                x = jnp.concatenate(
                    [
                        jnp.concatenate(
                            [
                                ring[slot, plane, a, pl.ds(base + g * block, block), pl.ds(c * LANES, LANES)]
                                for c in range(chunks)
                                for plane in range(2)
                            ],
                            0,
                        )
                        for g in range(2)
                    ],
                    1,
                )
                y = dot(spread[...], x)
                for g in range(2):
                    rows = y[:, g * LANES : (g + 1) * LANES].reshape(block, kinds, LANES)
                    table[pl.ds((s * step_rows + a) * cols + base + g * block, block)] = rows.astype(table.dtype)

    def turn_step(s, _):
        @pl.when(s + slots - 1 < steps)
        def _():
            fetch(s + slots - 1, lax.rem(s + slots - 1, slots)).start()

        turn(s)
        return 0

    early, late = EARLY, max(EARLY, steps * 3 // 8)
    ready = [min(steps, late + k) for k in range(FIRST // FAR)]
    lax.fori_loop(0, early, turn_step, 0)
    pl.semaphore_wait(barrier, len(peers) + len(others))
    ask = [
        remote(asked.at[level], got.at[level], idx_send.at[level], idx_recv.at[level], partner[level])
        for level in range(levels)
    ]
    for copy in ask:
        copy.start()
    lax.fori_loop(early, late, turn_step, 0)

    def slot_matrix(place):
        at = lax.broadcasted_iota(jnp.int32, (room, LANES), 0)
        for i in range(packs):
            mine = place[i : i + 1, :].astype(jnp.int32)
            hot[:, pl.ds(i * LANES, LANES)] = jnp.where(at == mine, one, nil).astype(hot.dtype)

    def by_slot(lists):
        parts = []
        for rows in lists:
            flat = blank - jnp.concatenate([rows[i : i + 1, :] for i in range(packs)], 1)
            parts += [flat // LANES, lax.rem(flat, LANES)]
        parts.append(jnp.zeros((8 - len(parts), count), jnp.int32))
        digits = jnp.concatenate(parts, 0).astype(jnp.float32).astype(jnp.bfloat16)
        moved = lax.dot_general(digits, hot[...], (((1,), (1,)), ((), ())), preferred_element_type=jnp.float32)
        out = []
        for i in range(len(lists)):
            value = moved[2 * i : 2 * i + 1] * LANES + moved[2 * i + 1 : 2 * i + 2]
            out.append(jnp.clip(blank - value.astype(jnp.int32), 0, blank))
        return out

    ask[last].wait()
    for i in range(packs):
        row = got[last, pl.ds(i, 1), :]
        good_out[last, pl.ds(i, 1), :] = look_up(row // cols, (lax.rem(row, cols),))
    good = good_out[last]
    antenna = got[last] // cols
    low = lax.broadcasted_iota(jnp.int32, (LANES, LANES), 0)
    high = lax.broadcasted_iota(jnp.int32, (LANES, LANES), 1)
    ahead_of = jnp.where(low < high, one, nil).astype(jnp.bfloat16)
    every = jnp.ones((LANES, LANES), jnp.bfloat16)
    number = lax.broadcasted_iota(jnp.int32, (dishes, LANES), 0)
    running, seen = jnp.zeros((dishes, LANES), jnp.float32), []
    for i in range(packs):
        mine = jnp.where(number == antenna[i : i + 1, :], good[i : i + 1, :], 0.0)
        mark = mine.astype(jnp.bfloat16)
        seen.append((mine, running + dot(mark, ahead_of)))
        running = running + dot(mark, every)
    row = lax.broadcasted_iota(jnp.int32, (dishes, dishes), 0)
    column = lax.broadcasted_iota(jnp.int32, (dishes, dishes), 1)
    offset = lax.dot_general(
        jnp.where(column < row, one, nil),
        running,
        (((1,), (0,)), ((), ())),
        precision=lax.Precision.HIGHEST,
        preferred_element_type=jnp.float32,
    )
    place = jnp.concatenate([jnp.sum(mine * (at + offset), 0, keepdims=True) for mine, at in seen], 0)
    place = jnp.where(good > 0.5, place, float(2 * count))
    used = jnp.sum(running, 0, keepdims=True)
    fits = used <= float(room)
    for k, done in enumerate(ready, 1):
        soon = jnp.sum(jnp.where(number < done * step_rows, running, 0.0), 0, keepdims=True)
        fits = fits & (soon >= jnp.minimum(used, float(k * FAR)))
    excess[...] = jnp.where(fits, nil, one)
    good_out[last] = place
    slot_matrix(place)
    (rows,) = by_slot([got[last]])
    far_rows[...] = jnp.full(far_rows.shape, blank, far_rows.dtype)
    for i in range(room // LANES):
        far_rows[pl.ds(i, 1), :] = rows[:, i * LANES : (i + 1) * LANES]
    moves = []
    for level in reversed(range(levels)):
        if level < last:
            ask[level].wait()
        rows = far_rows if level == last else got.at[level]
        moves.append(pltpu.make_async_copy(rows, ask_smem.at[level], move_sem.at[level]))
        moves[-1].start()

    def take(level, start, n):
        unroll = 32

        def some(it, _):
            at = start + it * unroll
            pack, lane = at // LANES, lax.rem(at, LANES)
            for u in range(unroll):
                bc_send[level, at + u] = table[ask_smem[level, pack, lane + u]]
            return 0

        lax.fori_loop(0, n // unroll, some, 0)

    far = [
        remote(
            bc_send.at[last, pl.ds(k * FAR, FAR)],
            bc_recv.at[last, pl.ds(k * FAR, FAR)],
            far_send.at[k],
            far_recv.at[k],
            partner[last],
        )
        for k in range(pieces)
    ]
    near = [
        remote(bc_send.at[level], bc_recv.at[level], near_send.at[level], near_recv.at[level], partner[level])
        for level in range(last)
    ]
    send_good = [
        remote(good_out.at[level], good_in.at[level], good_send.at[level], good_recv.at[level], partner[level])
        for level in range(levels)
    ]

    def look_up_asked(level):
        for i in range(packs):
            row = got[level, pl.ds(i, 1), :]
            good_out[level, pl.ds(i, 1), :] = look_up(row // cols, (lax.rem(row, cols),))

    for move in moves:
        move.wait()
    at = late
    for k, done in enumerate(ready):
        lax.fori_loop(at, done, turn_step, 0)
        at = done
        take(last, k * FAR, FAR)
        far[k].start()
        if k == 0:
            send_good[last].start()
    lax.fori_loop(at, steps, turn_step, 0)
    for k in range(FIRST // FAR, pieces):
        take(last, k * FAR, FAR)
        if k > FIRST // FAR:
            far[k - 1].start()
    for level in range(last):
        look_up_asked(level)
        take(level, 0, count)
        if level == 0:
            far[pieces - 1].start()
        send_good[level].start()
    goods = []
    for level in range(last):
        for i in range(packs):
            at = level * count + i * LANES
            a, b, c = [tri[pl.ds(e, 1), pl.ds(at, LANES)] for e in range(3)]
            goods.append(look_up(a - me * dishes, (b, c)))
        near[level].start()
    for level in range(last):
        send_good[level].wait()
        for i in range(packs):
            at = level * count + i * LANES
            a, b, c = [tri[pl.ds(e, 1), pl.ds(at, LANES)] for e in range(3)]
            first = a - me * dishes
            good = goods[level * packs + i] * good_in[level, pl.ds(i, 1), :] > 0.5
            own_rows[level, 0, pl.ds(i, 1), :] = jnp.clip(jnp.where(good, first * cols + b, blank), 0, blank)
            own_rows[level, 1, pl.ds(i, 1), :] = jnp.clip(first * cols + c, 0, blank)
    send_good[last].wait()
    slot_matrix(good_in[last])
    lists = [[], []]
    for i in range(packs):
        at = last * count + i * LANES
        a, b, c = [tri[pl.ds(e, 1), pl.ds(at, LANES)] for e in range(3)]
        first = a - me * dishes
        lists[0].append(first * cols + b)
        lists[1].append(first * cols + c)
    for e, rows in enumerate(by_slot([jnp.concatenate(rows, 0) for rows in lists])):
        own_rows[last, e] = jnp.full((packs, LANES), blank, jnp.int32)
        for i in range(room // LANES):
            own_rows[last, e, pl.ds(i, 1), :] = rows[:, i * LANES : (i + 1) * LANES]
    move_own = pltpu.make_async_copy(own_rows, own_smem, move_sem.at[levels])
    move_own.start()
    move_own.wait()

    def products(level, n_blocks, n):
        def some(it, _):
            for s in range(n_blocks):
                start = (it * n_blocks + s) * block
                pack, lane = start // LANES, lax.rem(start, LANES)
                for u in range(block):
                    for e in range(2):
                        row = table[own_smem[level, e, pack, lane + u]]
                        pair[s, e, pl.ds(u * kinds, kinds), :] = row
            for s in range(n_blocks):
                start = pl.multiple_of((it * n_blocks + s) * block, block)
                y = dot(gather[...], jnp.concatenate([pair[s, 0], pair[s, 1]], 1))
                for c in range(chunks):
                    at = 2 * c * block
                    a_r, a_i = y[at : at + block, :LANES], y[at + block : at + 2 * block, :LANES]
                    c_r, c_i = y[at : at + block, LANES:], y[at + block : at + 2 * block, LANES:]
                    prod[level, 0, c, pl.ds(start, block), :] = a_r * c_r + a_i * c_i
                    prod[level, 1, c, pl.ds(start, block), :] = a_i * c_r - a_r * c_i
            return 0

        lax.fori_loop(0, n // (n_blocks * block), some, 0)

    def bispectra(level, start, n):
        wide = min(2, n // block)
        acc = [None] * (3 * chunks)
        for s in range(n // (wide * block)):
            begin = pl.multiple_of(start + s * wide * block, wide * block)
            x = [bc_recv[level, pl.ds(begin + g * block, block)].reshape(SIDE, LANES) for g in range(wide)]
            y = dot(gather[...], jnp.concatenate(x, 1) if wide > 1 else x[0])
            for g in range(wide):
                lanes = slice(g * LANES, (g + 1) * LANES)
                rows = pl.ds(begin + g * block, block)
                total_r = total_i = None
                for c in range(chunks):
                    at = 2 * c * block
                    b_r, b_i = y[at : at + block, lanes], y[at + block : at + 2 * block, lanes]
                    w_r, w_i = prod[level, 0, c, rows, :], prod[level, 1, c, rows, :]
                    real = w_r * b_r - w_i * b_i
                    imag = w_r * b_i + w_i * b_r
                    norm = jnp.sqrt(real * real + imag * imag)
                    for part, value in enumerate((real, imag, norm)):
                        value = fold(value)
                        old = acc[3 * c + part]
                        acc[3 * c + part] = value if old is None else old + value
                    total_r = real if c == 0 else total_r + real
                    total_i = imag if c == 0 else total_i + imag
                line[0, pl.ds(s * wide * block + g * block, block), :] = total_r
                line[1, pl.ds(s * wide * block + g * block, block), :] = total_i
        for c in range(chunks):
            for part in range(3):
                spec_acc[c, part] = spec_acc[c, part] + acc[3 * c + part]
        ones = jnp.ones((8, LANES), jnp.float32)
        for part in range(2):
            lane_sum = lax.dot_general(
                ones,
                line[part, pl.ds(0, n), :],
                (((1,), (1,)), ((), ())),
                precision=lax.Precision.HIGHEST,
                preferred_element_type=jnp.float32,
            )
            sums[0, level, pl.ds(part, 1), pl.ds(pl.multiple_of(start, LANES), n)] = lane_sum[:1]

    for level in range(levels):
        products(level, 4 * 32 // block, room if level == last else count)
    for level in range(last):
        near[level].wait()
        lax.fori_loop(0, count // 256, lambda it, _, level=level: (bispectra(level, it * 256, 256), 0)[1], 0)
    ahead = [
        remote(sums.at[0, level], sums.at[k, level], sum_send.at[k, level], sum_recv.at[k, level], device)
        for k, device in enumerate(peers, 1)
        for level in range(last)
    ]
    for k in range(pieces):
        far[k].wait()
        bispectra(last, k * FAR, FAR)
        if k == 0:
            for copy in ahead:
                copy.start()
    copies = list(ahead)
    for k, device in enumerate(peers, 1):
        whole = pl.ds(0, room)
        copies.append(
            remote(
                sums.at[0, last, :, whole],
                sums.at[k, last, :, whole],
                sum_send.at[k, last],
                sum_recv.at[k, last],
                device,
            )
        )
        copies[-1].start()
    for c in range(chunks):
        for part in range(3):
            spec_out[c, pl.ds(part, 1), :] = jnp.sum(spec_acc[c, part], 0, keepdims=True)
        spec_out[c, pl.ds(3, 1), :] = excess[...]
    spread_out = []
    for k, device in enumerate(others, 1):
        spread_out.append(
            remote(
                spec_out.at[device[1] * width // LANES],
                spec_recv.at[k],
                spec_send_sem.at[k],
                spec_recv_sem.at[k],
                device,
            )
        )
        spread_out[-1].start()
    for copy in copies:
        copy.wait()
    bands = channels * groups
    for level in range(levels):
        n = room if level == last else count
        total = sums[0, level, :, pl.ds(0, n)]
        for k in range(1, groups):
            total = total + sums[k, level, :, pl.ds(0, n)]
        total = total / bands
        if level == last:
            parts, rest = [], total
            for _ in range(3):
                parts.append(rest.astype(jnp.bfloat16).astype(jnp.float32))
                rest = rest - parts[-1]
            parts.append(jnp.zeros((2, room), jnp.float32))
            moved = dot(jnp.concatenate(parts, 0).astype(jnp.bfloat16), hot[...])
            total = moved[0:2] + moved[2:4] + moved[4:6]
        means[:, pl.ds(level * count, count)] = total
    for copy in spread_out:
        copy.wait()
    total = spec_out[me * width // LANES]
    for k in range(1, tiles):
        total = total + spec_recv[k]
    closure[...] = total[:2] / (1.0 + total[2:3])
    missed[0] = jnp.max(total[3:4]).astype(jnp.int32)


def body(visibility, dish_pair_okay, triangles):
    _, dishes, cols, channels = visibility.shape
    levels = triangles.shape[1] // TRI_LVL
    tiles, groups = lax.axis_size("tile"), lax.axis_size("grp")
    chunks = channels // LANES
    kinds = 2 * chunks
    packs = TRI_LVL // LANES
    step_rows, slots = 4, 3
    room = far_room(TRI_LVL)
    pieces = room // FAR
    width = channels // tiles
    vmem = pl.BlockSpec(memory_space=pltpu.VMEM)
    f32, bf16, i32 = jnp.float32, jnp.bfloat16, jnp.int32
    dma = pltpu.SemaphoreType.DMA
    triangle_means, closure, missed = pl.pallas_call(
        functools.partial(mega_kernel, groups=groups, tiles=tiles, levels=levels, step_rows=step_rows),
        in_specs=[pl.BlockSpec(memory_space=pl.ANY), vmem, vmem],
        out_specs=[vmem, vmem, pl.BlockSpec(memory_space=pltpu.SMEM)],
        out_shape=[
            jax.ShapeDtypeStruct((2, triangles.shape[1]), f32),
            jax.ShapeDtypeStruct((2, LANES), f32),
            jax.ShapeDtypeStruct((1,), i32),
        ],
        scratch_shapes=[
            pltpu.VMEM((dishes * cols + 1, kinds, LANES), bf16),
            pltpu.VMEM((slots, 2, step_rows, cols, channels), bf16),
            pltpu.VMEM((SIDE, SIDE), bf16),
            pltpu.VMEM((SIDE, SIDE), bf16),
            pltpu.VMEM((levels, packs, LANES), i32),
            pltpu.VMEM((levels, packs, LANES), i32),
            pltpu.VMEM((levels, packs, LANES), f32),
            pltpu.VMEM((levels, packs, LANES), f32),
            pltpu.VMEM((packs, LANES), i32),
            pltpu.VMEM((room, TRI_LVL), bf16),
            pltpu.VMEM((1, LANES), f32),
            pltpu.VMEM((levels, 2, packs, LANES), i32),
            pltpu.SMEM((levels, packs, LANES), i32),
            pltpu.SMEM((levels, 2, packs, LANES), i32),
            pltpu.VMEM((levels, TRI_LVL, kinds, LANES), bf16),
            pltpu.VMEM((levels, TRI_LVL, kinds, LANES), bf16),
            pltpu.VMEM((4, 2, SIDE, LANES), bf16),
            pltpu.VMEM((levels, 2, chunks, TRI_LVL, LANES), f32),
            pltpu.VMEM((2, 256, LANES), f32),
            pltpu.VMEM((groups, levels, 2, TRI_LVL), f32),
            pltpu.VMEM((chunks, 3, 8, LANES), f32),
            pltpu.VMEM((chunks, 8, LANES), f32),
            pltpu.VMEM((tiles, 8, LANES), f32),
            dma((slots,)),
            dma((levels + 1,)),
            dma((levels,)),
            dma((levels,)),
            dma((levels,)),
            dma((levels,)),
            dma((levels,)),
            dma((levels,)),
            dma((pieces,)),
            dma((pieces,)),
            dma((groups, levels)),
            dma((groups, levels)),
            dma((tiles,)),
            dma((tiles,)),
        ],
        compiler_params=pltpu.CompilerParams(
            collective_id=0, has_side_effects=True, vmem_limit_bytes=67043328
        ),
        name="bispectra",
    )(visibility, dish_pair_okay, triangles)
    at = lax.rem(lax.axis_index("tile") * width, LANES)
    return lax.cond(
        missed[0] > 0,
        lambda: every_row(visibility, dish_pair_okay, triangles),
        lambda: (triangle_means, lax.dynamic_slice(closure, (0, at), (2, width))),
    )


def every_row(visibility, dish_pair_okay, triangles):
    _, dishes, cols, channels = visibility.shape
    levels = triangles.shape[1] // TRI_LVL
    tiles, groups = lax.axis_size("tile"), lax.axis_size("grp")
    device = lax.axis_index("tile")
    table = visibility.reshape(2, dishes * cols, channels)
    flags = dish_pair_okay.reshape(-1).astype(jnp.float32)
    means, spectrum = [], 0.0
    for level in range(levels):
        pairs = [(i, i ^ 1 << level) for i in range(tiles)]
        a, b, c = triangles[:, level * TRI_LVL : (level + 1) * TRI_LVL]
        first = (a - device * dishes) * cols
        asked = (b - jnp.bitwise_xor(device, 1 << level) * dishes) * cols + c
        asked = lax.ppermute(asked, "tile", pairs)
        bc = lax.ppermute(table[:, asked], "tile", pairs).astype(jnp.float32)
        weight = lax.ppermute(flags[asked], "tile", pairs) * flags[first + b] * flags[first + c]
        ab, ac = [table[:, first + x].astype(jnp.float32) for x in (b, c)]
        p_r, p_i = ab[0] * bc[0] - ab[1] * bc[1], ab[0] * bc[1] + ab[1] * bc[0]
        real = weight[:, None] * (p_r * ac[0] + p_i * ac[1])
        imag = weight[:, None] * (p_i * ac[0] - p_r * ac[1])
        norm = jnp.sqrt(real * real + imag * imag)
        spectrum = spectrum + jnp.stack([x.sum(0) for x in (real, imag, norm)])
        means.append(jnp.stack([x.sum(1) for x in (real, imag)]))
    means = lax.psum(jnp.concatenate(means, 1), "grp") / (channels * groups)
    spectrum = lax.psum(spectrum, "tile")
    closure = spectrum[:2] / (1.0 + spectrum[2])
    width = channels // tiles
    return means, lax.dynamic_slice_in_dim(closure, device * width, width, 1)


def solution(mesh):
    return jax.shard_map(
        body,
        mesh=mesh,
        in_specs=(P(None, "tile", None, "grp"), P("tile", None), P(None, "tile")),
        out_specs=(P(None, "tile"), P(None, ("grp", "tile"))),
        check_vma=False,
    )
```
